32 devices in a mesh: gx: 2 (over x), gy: 4 (over z), gz: 4 (over y, core).
Axes of the slice: x: 2, y: 2, z: 4, core: 2. Of those that a mesh axis runs over, the one named last changes fastest.
Arguments:
- right_side: float32 [128, 256, 1024], P('gx', 'gy', 'gz'), may hold values from -5 to 7
- initial_guess: float32 [128, 256, 1024], P('gx', 'gy', 'gz'), may hold values from -5 to 7
Outputs:
- solution: float32 [128, 256, 1024], P('gx', 'gy', 'gz')
The draws below stay inside these ranges and needn't reach their ends.
All inputs are finite; a program needn't handle non-finite values.
Results may differ from the reference program's by a relative error of at most 0.000028.
Values sent between devices are 32-bit elements; how exact they have to be, the bound alone decides.
A program may use at most 128 MiB of HBM per device.

```python
import jax
import jax.numpy as jnp

COARSE_SWEEPS = 6
NX = 128
NY = 256
NZ = 1024


def ramp_field(key, rising):
    noise = jnp.clip(jax.random.normal(key, (NX, NY, NZ), jnp.float32), -5.0, 5.0)
    position = jnp.arange(NX, dtype=jnp.float32) / NX
    if rising:
        offset = 0.5 + position
    else:
        offset = 1.5 - position
    return noise + offset[:, None, None]


def draw_right_side(key, part):
    return ramp_field(jax.random.fold_in(key, 11), True)


def draw_initial_guess(key, part):
    return ramp_field(jax.random.fold_in(key, 23), False)


def setup_inputs(seed: int = 0) -> dict:
    streams_of = jax.random.split(jax.random.key(seed), 3)
    return {
        "right_side": draw_right_side(jax.random.fold_in(streams_of[2], 71), 0),
        "initial_guess": draw_initial_guess(jax.random.fold_in(streams_of[2], 71), 0),
    }


relax_weight = 0.8


def neighbours(values):
    total = jnp.roll(values, -1, 0) + jnp.roll(values, 1, 0)
    total = total + jnp.roll(values, -1, 1) + jnp.roll(values, 1, 1)
    total = total + jnp.roll(values, -1, 2) + jnp.roll(values, 1, 2)
    return total


def relax_step(centre, beside, source, level_scale):
    return centre + relax_weight * (source / (6.0 * level_scale) - centre + beside / 6.0)


def defect_of(centre, beside, source, level_scale):
    return source - level_scale * (6.0 * centre - beside)


def restrict_grid(values):
    for along in range(3):
        count_half = values.shape[along] // 2
        on_points = jax.lax.slice_in_dim(values, 0, 2 * count_half, 2, along)
        between = jax.lax.slice_in_dim(values, 1, 2 * count_half, 2, along)
        lower_side = jnp.roll(between, 1, along)
        values = 0.25 * lower_side + 0.5 * on_points + 0.25 * between
    return values


def prolong_grid(values):
    for along in range(3):
        between = 0.5 * (values + jnp.roll(values, -1, along))
        stacked = jnp.stack([values, between], along + 1)
        new_shape = list(values.shape)
        new_shape[along] = 2 * new_shape[along]
        values = stacked.reshape(new_shape)
    return values


def smoothed(approx, source, level_scale):
    return relax_step(approx, neighbours(approx), source, level_scale)


def multigrid_cycle(approx, source, grid_level):
    level_scale = 0.25 ** grid_level
    if grid_level == 2:
        approx = smoothed(jnp.zeros_like(source), source, level_scale)
        for sweep_index in range(COARSE_SWEEPS - 1):
            approx = smoothed(approx, source, level_scale)
        return approx
    approx = smoothed(smoothed(approx, source, level_scale), source, level_scale)
    defect_field = defect_of(approx, neighbours(approx), source, level_scale)
    coarse_source = restrict_grid(defect_field)
    correction = multigrid_cycle(jnp.zeros_like(coarse_source), coarse_source, grid_level + 1)
    approx = approx + prolong_grid(correction)
    return smoothed(smoothed(approx, source, level_scale), source, level_scale)


def reference(right_side, initial_guess):
    cell_count = NX * NY * NZ
    source = right_side - jnp.sum(right_side) / cell_count
    approx = initial_guess - jnp.sum(initial_guess) / cell_count
    return multigrid_cycle(approx, source, 0)
```

```python
import functools
import itertools

import jax
import jax.numpy as jnp
from jax import lax
from jax.experimental import pallas as pl
from jax.experimental.pallas import tpu as pltpu
from jax.sharding import PartitionSpec as P

COARSE_SWEEPS = 6
LANES = 128
AXES = ("gx", "gy", "gz")
relax_weight = 0.8


def dot_exact(a, w):
    hi = a.astype(jnp.bfloat16)
    rest = a - hi.astype(jnp.float32)
    mid = rest.astype(jnp.bfloat16)
    low = (rest - mid.astype(jnp.float32)).astype(jnp.bfloat16)
    dot = functools.partial(jnp.dot, preferred_element_type=jnp.float32)
    return dot(hi, w) + (dot(mid, w) + dot(low, w))


def iotas(shape):
    return (
        lax.broadcasted_iota(jnp.int32, shape, 0),
        lax.broadcasted_iota(jnp.int32, shape, 1),
    )


def restrict_matrix(rows, cols, count, wrap=None):
    r, c = iotas((rows, cols))
    w = jnp.where(r == 2 * c, 0.5, 0.0) + jnp.where(jnp.abs(r - 2 * c) == 1, 0.25, 0.0)
    w = jnp.where((c < count) & (r < 2 * count), w, 0.0)
    if wrap is not None:
        w = w + jnp.where((r == wrap) & (c == 0), 0.25, 0.0)
    return w.astype(jnp.bfloat16)


def prolong_matrix(rows, cols, count):
    r, c = iotas((rows, cols))
    w = jnp.where(c == 2 * r, 1.0, 0.0)
    w = w + jnp.where((c == 2 * r + 1) | (c == 2 * r - 1), 0.5, 0.0)
    return jnp.where(r < count, w, 0.0).astype(jnp.bfloat16)


def lane_pad(z):
    return max(z, LANES)


def turn(by):
    return by % LANES if isinstance(by, int) else lax.rem(by, LANES)


def tile_up(h, width):
    return jnp.concatenate([h] * (width // LANES), 1) if width > LANES else h


def buffers(dims):
    f32 = jnp.float32
    out = {}
    rounds = (5, 4, COARSE_SWEEPS - 1)
    for l, (x, y, z) in enumerate(dims):
        zl = lane_pad(z)
        for name in "AB":
            out[f"{name}{l}"] = (x, y, zl)
        if l:
            out[f"G{l}"] = (x, y, zl)
        out[f"yp{l}"] = (2, x, zl)
        out[f"zp{l}"] = (2, y, LANES)
        out[f"hx{l}"] = (rounds[l], 2, y, zl)
        out[f"hy{l}"] = (rounds[l], 2, x, zl)
        out[f"hz{l}"] = (rounds[l], 2, y, LANES)
        for kind in (["r"] if l < 2 else []) + (["p"] if l else []):
            out[f"{kind}x{l}"] = (y, zl)
            out[f"{kind}y{l}"] = (x + 8, zl)
            out[f"{kind}z{l}"] = (y + 8, LANES)
            out[f"{kind}w{l}"] = (y + 8, LANES)
        if l < 2:
            out[f"T{l}"] = (x // 2, y // 2, zl)
            out[f"S{l}"] = (zl // LANES, y, LANES)
            out[f"TH{l}"] = (y // 2, zl)
            out[f"TY{l}"] = (x // 2 + 8, zl)
        out[f"M{l}"] = (y + 8, LANES)
        out[f"N{l}"] = (y, LANES)
    return {k: pltpu.VMEM(v, f32) for k, v in out.items()}


def kernel(dims, counts, names, cells, u, f, out, *scratch):
    b = dict(zip(names, scratch[:-2]))
    send_sem, recv_sem = scratch[-2:]
    here = {a: lax.axis_index(a) for a in AXES}
    serial = itertools.count()

    def device(offset):
        return tuple(lax.rem(here[a] + (o % n), n) for a, o, n in zip(AXES, offset, counts))

    def copy(src, dst, offset):
        k = next(serial)
        c = pltpu.make_async_remote_copy(
            src_ref=src,
            dst_ref=dst,
            send_sem=send_sem.at[k],
            recv_sem=recv_sem.at[k],
            device_id=device(offset),
            device_id_type=pl.DeviceIdType.MESH,
        )
        c.start()
        return c

    def wait(copies):
        for c in copies:
            c.wait()

    offsets = []
    for sign in (1, -1):
        for o in itertools.product((0, 1), repeat=3):
            if any(o):
                offsets.append(tuple(sign * v for v in o))
    for a in range(3):
        for j in range(2, counts[a] - 1):
            offsets.append(tuple(j if i == a else 0 for i in range(3)))
    barrier = pltpu.get_barrier_semaphore()
    for o in offsets:
        pl.semaphore_signal(
            barrier, inc=1, device_id=device(o), device_id_type=pl.DeviceIdType.MESH
        )
    pl.semaphore_wait(barrier, len(offsets))

    def exchange(l, r, v):
        x = dims[l][0]
        hx, hy, hz = (b[f"h{a}{l}"] for a in "xyz")
        yp, zp = b[f"yp{l}"], b[f"zp{l}"]
        return [
            copy(yp.at[1], hy.at[r, 0], (0, 1, 0)),
            copy(yp.at[0], hy.at[r, 1], (0, -1, 0)),
            copy(zp.at[1], hz.at[r, 0], (0, 0, 1)),
            copy(zp.at[0], hz.at[r, 1], (0, 0, -1)),
            copy(v.at[x - 1], hx.at[r, 0], (1, 0, 0)),
            copy(v.at[0], hx.at[r, 1], (-1, 0, 0)),
        ]

    def corner_exchange(kind, l, v):
        x, y, _ = dims[l]
        hi = kind == "r"
        s = 1 if hi else -1
        side = 1 if hi else 0
        yp, zp = b[f"yp{l}"].at[side], b[f"zp{l}"].at[side]
        hx, hy, hz, hw = (b[f"{kind}{a}{l}"] for a in "xyzw")
        ye = yp.at[pl.ds(x - 8 if hi else 0, 8)]
        ze = zp.at[pl.ds(y - 8 if hi else 0, 8)]
        return [
            copy(ze, hw.at[pl.ds(y, 8)], (s, s, s)),
            copy(zp, hw.at[pl.ds(0, y)], (s, 0, s)),
            copy(ze, hz.at[pl.ds(y, 8)], (0, s, s)),
            copy(ye, hy.at[pl.ds(x, 8)], (s, s, 0)),
            copy(yp, hy.at[pl.ds(0, x)], (0, s, 0)),
            copy(zp, hz.at[pl.ds(0, y)], (0, 0, s)),
            copy(v.at[x - 1 if hi else 0], hx, (s, 0, 0)),
        ]

    def zero_acc(l):
        z = jnp.zeros((dims[l][1], LANES), jnp.float32)
        return (z, z)

    def pack(l, x, new, acc):
        _, y, z = dims[l]
        yp = b[f"yp{l}"]
        yp[0, pl.ds(x, 1), :] = new[:1]
        yp[1, pl.ds(x, 1), :] = new[y - 1 :]
        lane = lax.broadcasted_iota(jnp.int32, (y, LANES), 1)
        last = (z - 1) % LANES
        low = pltpu.roll(new[:, :LANES], x, 1)
        high = pltpu.roll(new[:, -LANES:], turn(x + (LANES - last)), 1)
        return (jnp.where(lane == x, low, acc[0]), jnp.where(lane == x, high, acc[1]))

    def store_acc(l, acc):
        b[f"zp{l}"][0] = acc[0]
        b[f"zp{l}"][1] = acc[1]

    def planes(l, body, packed=True):
        def step(i, acc):
            new = body(i)
            return pack(l, i, new, acc) if packed else acc

        acc = lax.fori_loop(0, dims[l][0], step, zero_acc(l))
        if packed:
            store_acc(l, acc)

    def sweep(l, r, src, dst, g, defect=False, shift=None, packed=True):
        x, y, z = dims[l]
        zl = lane_pad(z)
        scale = 0.25**l
        hx, hy, hz = (b[f"h{a}{l}"].at[r] for a in "xyz")
        row, lane = iotas((y, zl))
        last = (z - 1) % LANES

        def plane(i, before, after, acc):
            c = src[i]
            up = jnp.where(row == 0, hy[0, pl.ds(i, 1), :], pltpu.roll(c, 1, 0))
            down = jnp.where(row == y - 1, hy[1, pl.ds(i, 1), :], pltpu.roll(c, y - 1, 0))
            left = pltpu.roll(hz[0], turn(LANES - i), 1)
            left = jnp.where(lane == 0, tile_up(left, zl), pltpu.roll(c, 1, 1))
            right = pltpu.roll(hz[1], turn(LANES + last - i), 1)
            right = jnp.where(lane == z - 1, tile_up(right, zl), pltpu.roll(c, zl - 1, 1))
            beside = (after + before) + (up + down) + (left + right)
            if defect:
                new = g[i] - scale * (6.0 * c - beside)
            else:
                new = (1.0 - relax_weight) * c + (relax_weight / 6.0) * beside
                new = new + (relax_weight / (6.0 * scale)) * g[i]
                if shift is not None:
                    new = new - shift
            dst[i] = new
            return pack(l, i, new, acc) if packed else acc

        def inner(i, acc):
            return plane(i, src[i - 1], src[i + 1], acc)

        acc = plane(0, hx[0], src[1], zero_acc(l))
        acc = lax.fori_loop(1, x - 1, inner, acc)
        acc = plane(x - 1, src[x - 2], hx[1], acc)
        if packed:
            store_acc(l, acc)

    def halves(v):
        return [v[:, k : k + LANES] for k in range(0, v.shape[1], LANES)]

    def restrict_y(ref, row_before):
        n = ref.shape[1] // 2
        parts = []
        first = lax.broadcasted_iota(jnp.int32, (n, LANES), 0) == 0
        for t, rim in enumerate(halves(row_before)):
            even = ref[t, pl.ds(0, n, stride=2), :]
            odd = ref[t, pl.ds(1, n, stride=2), :]
            below = jnp.where(first, rim, pltpu.roll(odd, 1, 0))
            parts.append(0.25 * below + 0.5 * even + 0.25 * odd)
        return jnp.concatenate(parts, 1) if len(parts) > 1 else parts[0]

    def restrict_down(l, d, mean):
        x, y, z = dims[l]
        zl = lane_pad(z)
        xc, yc, zc = dims[l + 1]
        zlc = lane_pad(zc)
        hx, hy, hz, hw = (b[f"r{a}{l}"] for a in "xyzw")
        s, t = b[f"S{l}"], b[f"T{l}"]
        m, n = b[f"M{l}"], b[f"N{l}"]
        lane = lax.broadcasted_iota(jnp.int32, (y + 8, LANES), 1)
        moved = pltpu.roll(hw[...], LANES - x, 1)
        rim = jnp.where(lane == LANES - 1, moved, hz[...])
        m[...] = dot_exact(rim, restrict_matrix(LANES, LANES, xc, LANES - 1))
        n[...] = m[pl.ds(0, y), :]
        even = n[pl.ds(0, yc, stride=2), :]
        odd = n[pl.ds(1, yc, stride=2), :]
        first = lax.broadcasted_iota(jnp.int32, (yc, LANES), 0) == 0
        below = jnp.where(first, m[pl.ds(y + 7, 1), :], pltpu.roll(odd, 1, 0))
        n[pl.ds(0, yc), :] = 0.25 * (0.25 * below + 0.5 * even + 0.25 * odd)

        def plane(i, before, before_row):
            dx = 0.25 * before + 0.5 * d[2 * i] + 0.25 * d[2 * i + 1]
            for k, part in enumerate(halves(dx)):
                s[k] = part
            rows = 0.25 * before_row + 0.5 * hy[pl.ds(2 * i, 1), :]
            rows = rows + 0.25 * hy[pl.ds(2 * i + 1, 1), :]
            t[i] = restrict_y(s, rows)

        def inner(i, _):
            plane(i, d[2 * i - 1], hy[pl.ds(2 * i - 1, 1), :])
            return 0

        plane(0, hx[...], hy[pl.ds(x + 7, 1), :])
        lax.fori_loop(1, xc, inner, 0)
        g, v = b[f"G{l + 1}"], b[f"A{l + 1}"]
        w = restrict_matrix(zl, zlc, zc)
        chunk = 8

        def multiply(k, _):
            rows = t[pl.ds(k * chunk, chunk)].reshape(chunk * yc, zl)
            g[pl.ds(k * chunk, chunk)] = dot_exact(rows, w).reshape(chunk, yc, zlc)
            return 0

        lax.fori_loop(0, xc // chunk, multiply, 0)
        lane_c = lax.broadcasted_iota(jnp.int32, (yc, zlc), 1)

        def finish(i):
            col = pltpu.roll(n[pl.ds(0, yc), :], turn(LANES - i), 1)
            new = g[i] + jnp.where(lane_c == 0, tile_up(col, zlc), 0.0)
            if mean is not None:
                new = new - mean
            g[i] = new
            new = (relax_weight / (6.0 * 0.25 ** (l + 1))) * new
            v[i] = new
            return new

        planes(l + 1, finish)

    def prolong_up(l, c, v, work, shift):
        x, y, z = dims[l]
        zl = lane_pad(z)
        xc, yc, zc = dims[l + 1]
        zlc = lane_pad(zc)
        hx, hy, hz, hw = (b[f"p{a}{l + 1}"] for a in "xyzw")
        s, t, th, ty = b[f"S{l}"], b[f"T{l}"], b[f"TH{l}"], b[f"TY{l}"]
        m = b[f"M{l + 1}"]
        lane = lax.broadcasted_iota(jnp.int32, (yc + 8, LANES), 1)
        m[...] = 0.5 * jnp.where(lane == xc, pltpu.roll(hw[...], xc, 1), hz[...])
        w = prolong_matrix(zlc, zl, zc)
        chunk = 8

        def multiply(k, _):
            rows = c[pl.ds(k * chunk, chunk)].reshape(chunk * yc, zlc)
            t[pl.ds(k * chunk, chunk)] = dot_exact(rows, w).reshape(chunk, yc, zl)
            return 0

        lax.fori_loop(0, xc // chunk, multiply, 0)
        th[...] = dot_exact(hx[...], w)
        ty[...] = dot_exact(hy[...], w)
        at_end = lane == LANES - 1
        final = lax.broadcasted_iota(jnp.int32, (yc, LANES), 0) == yc - 1

        def plane(i, values):
            add = pltpu.roll(m[...], turn(2 * LANES - 1 - i), 1)
            add = jnp.where(at_end, add, 0.0)
            rim = ty[pl.ds(i, 1), :]
            rims, parts = halves(rim), halves(values)
            parts[-1] = parts[-1] + add[:yc]
            rims[-1] = rims[-1] + add[yc : yc + 1]
            for k, (part, edge) in enumerate(zip(parts, rims)):
                above = jnp.where(final, edge, pltpu.roll(part, yc - 1, 0))
                s[k, pl.ds(0, yc, stride=2), :] = part
                s[k, pl.ds(1, yc, stride=2), :] = 0.5 * (part + above)
            full = [s[k] for k in range(len(parts))]
            work[i] = jnp.concatenate(full, 1) if len(full) > 1 else full[0]

        def spread(i, _):
            plane(i, t[i])
            return 0

        lax.fori_loop(0, xc, spread, 0)
        plane(xc, th[...])

        def add(i, acc):
            low, high = work[i], work[i + 1]
            if shift is not None:
                low, high = low - shift, high - shift
            even = v[2 * i] + low
            odd = v[2 * i + 1] + 0.5 * (low + high)
            v[2 * i] = even
            v[2 * i + 1] = odd
            return pack(l, 2 * i + 1, odd, pack(l, 2 * i, even, acc))

        store_acc(l, lax.fori_loop(0, xc, add, zero_acc(l)))

    st, sg = b["stats"], [b[f"sums{a}"] for a in range(3)]

    def spread_sums(a):
        return [
            copy(st.at[a], sg[a].at[j], tuple(j if i == a else 0 for i in range(3)))
            for j in range(1, counts[a])
        ]

    def gather_sums(a, copies):
        wait(copies)
        total = st[a]
        for j in range(1, counts[a]):
            total = total + sg[a][j]
        if a < 2:
            st[a + 1] = total
        return total

    x0, y0, z0 = dims[0]

    def folded(v):
        return jnp.sum(v.reshape(y0 // 8, 8, z0), 0)

    def first(i, carry):
        total, acc = carry
        v = u[i]
        return total + folded(v), pack(0, i, v, acc)

    none = jnp.zeros((8, z0), jnp.float32)
    total_u, acc = lax.fori_loop(0, x0, first, (none, zero_acc(0)))
    store_acc(0, acc)
    moving = exchange(0, 0, u)
    total_f = lax.fori_loop(0, x0, lambda i, t: t + folded(f[i]), none)
    st[0, 0] = total_u
    st[0, 1] = total_f
    sums = spread_sums(0)
    a0, b0, a1, b1 = b["A0"], b["B0"], b["A1"], b["B1"]
    a2, b2 = b["A2"], b["B2"]
    wait(moving)
    sweep(0, 0, u, a0, f)
    moving = exchange(0, 1, a0)
    gather_sums(0, sums)
    sums = spread_sums(1)
    wait(moving)
    sweep(0, 1, a0, b0, f)
    moving = exchange(0, 2, b0)
    gather_sums(1, sums)
    sums = spread_sums(2)
    wait(moving)
    sweep(0, 2, b0, a0, f, defect=True)
    moving = corner_exchange("r", 0, a0)
    total = gather_sums(2, sums)
    mean_u = jnp.sum(total[0]) * (1.0 / cells)
    mean_f = jnp.sum(total[1]) * (1.0 / cells)
    gain = relax_weight / 6.0
    wait(moving)
    restrict_down(0, a0, mean_f)

    wait(exchange(1, 0, a1))
    sweep(1, 0, a1, b1, b["G1"])
    wait(exchange(1, 1, b1))
    sweep(1, 1, b1, a1, b["G1"], defect=True)
    wait(corner_exchange("r", 1, a1))
    restrict_down(1, a1, None)

    v, w = a2, b2
    for k in range(COARSE_SWEEPS - 1):
        wait(exchange(2, k, v))
        sweep(2, k, v, w, b["G2"])
        v, w = w, v
    wait(corner_exchange("p", 2, v))
    prolong_up(1, v, b1, a1, None)
    wait(exchange(1, 2, b1))
    sweep(1, 2, b1, a1, b["G1"])
    wait(exchange(1, 3, a1))
    sweep(1, 3, a1, b1, b["G1"])
    wait(corner_exchange("p", 1, b1))
    prolong_up(0, b1, b0, a0, mean_u + 2.0 * gain * mean_f)
    wait(exchange(0, 3, b0))
    sweep(0, 3, b0, a0, f, shift=gain * mean_f)
    wait(exchange(0, 4, a0))
    sweep(0, 4, a0, out, f, shift=gain * mean_f, packed=False)


def solution(mesh):
    counts = tuple(mesh.shape[a] for a in AXES)

    def shards(right_side, initial_guess):
        shape = right_side.shape
        dims = tuple(tuple(n >> l for n in shape) for l in range(3))
        cells = float(right_side.size)
        for n in counts:
            cells *= n
        bufs = buffers(dims)
        bufs["stats"] = pltpu.VMEM((3, 2, 8, shape[2]), jnp.float32)
        for a in range(3):
            bufs[f"sums{a}"] = pltpu.VMEM((counts[a], 2, 8, shape[2]), jnp.float32)
        messages = 6 * (9 + COARSE_SWEEPS - 1) + 7 * 4 + sum(counts) - 3
        vmem = pl.BlockSpec(memory_space=pltpu.VMEM)
        return pl.pallas_call(
            functools.partial(kernel, dims, counts, tuple(bufs), cells),
            out_shape=jax.ShapeDtypeStruct(shape, jnp.float32),
            in_specs=[vmem, vmem],
            out_specs=vmem,
            scratch_shapes=list(bufs.values())
            + [pltpu.SemaphoreType.DMA((messages,)), pltpu.SemaphoreType.DMA((messages,))],
            compiler_params=pltpu.CompilerParams(
                collective_id=0, has_side_effects=True, vmem_limit_bytes=48 * 1024 * 1024
            ),
        )(initial_guess, right_side)

    placed = (P(*AXES), P(*AXES))
    return jax.shard_map(
        shards, mesh=mesh, in_specs=placed, out_specs=P(*AXES), check_vma=False
    )
```

```python
import functools
import itertools

import jax
import jax.numpy as jnp
from jax import lax
from jax.experimental import pallas as pl
from jax.experimental.pallas import tpu as pltpu
from jax.sharding import PartitionSpec as P

COARSE_SWEEPS = 6
LANES = 128
AXES = ("gx", "gy", "gz")
relax_weight = 0.8


def dot_exact(a, w):
    hi = a.astype(jnp.bfloat16)
    rest = a - hi.astype(jnp.float32)
    mid = rest.astype(jnp.bfloat16)
    low = (rest - mid.astype(jnp.float32)).astype(jnp.bfloat16)
    dot = functools.partial(jnp.dot, preferred_element_type=jnp.float32)
    return dot(hi, w) + (dot(mid, w) + dot(low, w))


def iotas(shape):
    return (
        lax.broadcasted_iota(jnp.int32, shape, 0),
        lax.broadcasted_iota(jnp.int32, shape, 1),
    )


def restrict_matrix(rows, cols, count, wrap=None):
    r, c = iotas((rows, cols))
    w = jnp.where(r == 2 * c, 0.5, 0.0) + jnp.where(jnp.abs(r - 2 * c) == 1, 0.25, 0.0)
    w = jnp.where((c < count) & (r < 2 * count), w, 0.0)
    if wrap is not None:
        w = w + jnp.where((r == wrap) & (c == 0), 0.25, 0.0)
    return w.astype(jnp.bfloat16)


def prolong_matrix(rows, cols, count):
    r, c = iotas((rows, cols))
    w = jnp.where(c == 2 * r, 1.0, 0.0)
    w = w + jnp.where((c == 2 * r + 1) | (c == 2 * r - 1), 0.5, 0.0)
    return jnp.where(r < count, w, 0.0).astype(jnp.bfloat16)


def lane_pad(z):
    return max(z, LANES)


def turn(by):
    return by % LANES if isinstance(by, int) else lax.rem(by, LANES)


def tile_up(h, width):
    return jnp.concatenate([h] * (width // LANES), 1) if width > LANES else h


def buffers(dims):
    f32 = jnp.float32
    out = {}
    rounds = (5, 4, COARSE_SWEEPS - 1)
    for l, (x, y, z) in enumerate(dims):
        zl = lane_pad(z)
        for name in "AB":
            out[f"{name}{l}"] = (x, y, zl)
        if l:
            out[f"G{l}"] = (x, y, zl)
        out[f"yp{l}"] = (2, x, zl)
        out[f"zp{l}"] = (2, y, LANES)
        out[f"hx{l}"] = (rounds[l], 2, y, zl)
        out[f"hy{l}"] = (rounds[l], 2, x, zl)
        out[f"hz{l}"] = (rounds[l], 2, y, LANES)
        for kind in (["r"] if l < 2 else []) + (["p"] if l else []):
            out[f"{kind}x{l}"] = (y, zl)
            out[f"{kind}y{l}"] = (x + 8, zl)
            out[f"{kind}z{l}"] = (y + 8, LANES)
            out[f"{kind}w{l}"] = (y + 8, LANES)
        if l < 2:
            out[f"T{l}"] = (x // 2, y // 2, zl)
            out[f"S{l}"] = (zl // LANES, y, LANES)
            out[f"TH{l}"] = (y // 2, zl)
            out[f"TY{l}"] = (x // 2 + 8, zl)
        out[f"M{l}"] = (y + 8, LANES)
        out[f"N{l}"] = (y, LANES)
    return {k: pltpu.VMEM(v, f32) for k, v in out.items()}


def kernel(dims, counts, names, cells, u, f, out, *scratch):
    b = dict(zip(names, scratch[:-2]))
    send_sem, recv_sem = scratch[-2:]
    here = {a: lax.axis_index(a) for a in AXES}
    serial = itertools.count()

    def device(offset):
        return tuple(lax.rem(here[a] + (o % n), n) for a, o, n in zip(AXES, offset, counts))

    def copy(src, dst, offset):
        k = next(serial)
        c = pltpu.make_async_remote_copy(
            src_ref=src,
            dst_ref=dst,
            send_sem=send_sem.at[k],
            recv_sem=recv_sem.at[k],
            device_id=device(offset),
            device_id_type=pl.DeviceIdType.MESH,
        )
        c.start()
        return c

    def wait(copies):
        for c in copies:
            c.wait()

    offsets = []
    for sign in (1, -1):
        for o in itertools.product((0, 1), repeat=3):
            if any(o):
                offsets.append(tuple(sign * v for v in o))
    for a in range(3):
        for j in range(2, counts[a] - 1):
            offsets.append(tuple(j if i == a else 0 for i in range(3)))
    barrier = pltpu.get_barrier_semaphore()
    for o in offsets:
        pl.semaphore_signal(
            barrier, inc=1, device_id=device(o), device_id_type=pl.DeviceIdType.MESH
        )
    pl.semaphore_wait(barrier, len(offsets))

    def exchange(l, r, v):
        x = dims[l][0]
        hx, hy, hz = (b[f"h{a}{l}"] for a in "xyz")
        yp, zp = b[f"yp{l}"], b[f"zp{l}"]

        def early():
            return [
                copy(v.at[x - 1], hx.at[r, 0], (1, 0, 0)),
                copy(v.at[0], hx.at[r, 1], (-1, 0, 0)),
            ]

        def late():
            return [
                copy(yp.at[1], hy.at[r, 0], (0, 1, 0)),
                copy(yp.at[0], hy.at[r, 1], (0, -1, 0)),
                copy(zp.at[1], hz.at[r, 0], (0, 0, 1)),
                copy(zp.at[0], hz.at[r, 1], (0, 0, -1)),
            ]

        return early, late

    def corner_exchange(kind, l, v):
        x, y, _ = dims[l]
        hi = kind == "r"
        s = 1 if hi else -1
        side = 1 if hi else 0
        yp, zp = b[f"yp{l}"].at[side], b[f"zp{l}"].at[side]
        hx, hy, hz, hw = (b[f"{kind}{a}{l}"] for a in "xyzw")
        ye = yp.at[pl.ds(x - 8 if hi else 0, 8)]
        ze = zp.at[pl.ds(y - 8 if hi else 0, 8)]

        def early():
            return [copy(v.at[x - 1 if hi else 0], hx, (s, 0, 0))]

        def late():
            return [
                copy(ze, hw.at[pl.ds(y, 8)], (s, s, s)),
                copy(zp, hw.at[pl.ds(0, y)], (s, 0, s)),
                copy(ze, hz.at[pl.ds(y, 8)], (0, s, s)),
                copy(ye, hy.at[pl.ds(x, 8)], (s, s, 0)),
                copy(yp, hy.at[pl.ds(0, x)], (0, s, 0)),
                copy(zp, hz.at[pl.ds(0, y)], (0, 0, s)),
            ]

        return early, late

    def both(parts):
        return parts[0]() + parts[1]()

    def zero_acc(l):
        z = jnp.zeros((dims[l][1], LANES), jnp.float32)
        return (z, z)

    def pack(l, x, new, acc):
        _, y, z = dims[l]
        yp = b[f"yp{l}"]
        yp[0, pl.ds(x, 1), :] = new[:1]
        yp[1, pl.ds(x, 1), :] = new[y - 1 :]
        lane = lax.broadcasted_iota(jnp.int32, (y, LANES), 1)
        last = (z - 1) % LANES
        low = pltpu.roll(new[:, :LANES], x, 1)
        high = pltpu.roll(new[:, -LANES:], turn(x + (LANES - last)), 1)
        return (jnp.where(lane == x, low, acc[0]), jnp.where(lane == x, high, acc[1]))

    def store_acc(l, acc):
        b[f"zp{l}"][0] = acc[0]
        b[f"zp{l}"][1] = acc[1]

    def planes(l, body, packed=True):
        def step(i, acc):
            new = body(i)
            return pack(l, i, new, acc) if packed else acc

        acc = lax.fori_loop(0, dims[l][0], step, zero_acc(l))
        if packed:
            store_acc(l, acc)

    def sweep(l, r, moving, src, dst, g, onward=None, defect=False, shift=None):
        x, y, z = dims[l]
        zl = lane_pad(z)
        scale = 0.25**l
        hx, hy, hz = (b[f"h{a}{l}"].at[r] for a in "xyz")
        row, lane = iotas((y, zl))
        last = (z - 1) % LANES
        gain = scale if defect else relax_weight / 6.0

        def plane(i, around):
            c = src[i]
            up = jnp.where(row == 0, 0.0, pltpu.roll(c, 1, 0))
            down = jnp.where(row == y - 1, 0.0, pltpu.roll(c, y - 1, 0))
            left = jnp.where(lane == 0, 0.0, pltpu.roll(c, 1, 1))
            right = jnp.where(lane == z - 1, 0.0, pltpu.roll(c, zl - 1, 1))
            beside = around + (up + down) + (left + right)
            if defect:
                new = g[i] - scale * (6.0 * c - beside)
            else:
                new = (1.0 - relax_weight) * c + (relax_weight / 6.0) * beside
                new = new + (relax_weight / (6.0 * scale)) * g[i]
                if shift is not None:
                    new = new - shift
            dst[i] = new

        def inner(i, _):
            plane(i, src[i - 1] + src[i + 1])
            return 0

        plane(0, src[1])
        lax.fori_loop(1, x - 1, inner, 0)
        plane(x - 1, src[x - 2])
        wait(moving)
        row8 = lax.broadcasted_iota(jnp.int32, (8, zl), 0)
        lane1 = lax.broadcasted_iota(jnp.int32, (y, LANES), 1)

        def fix(i, acc, beyond=None):
            new = dst[i]
            if beyond is not None:
                new = new + gain * beyond
            top = new[:8] + jnp.where(row8 == 0, gain * hy[0, pl.ds(i, 1), :], 0.0)
            new = jnp.concatenate([top, new[8:]], 0) if y > 8 else top
            end = new[y - 8 :] + jnp.where(row8 == 7, gain * hy[1, pl.ds(i, 1), :], 0.0)
            new = jnp.concatenate([new[: y - 8], end], 0) if y > 8 else end
            parts = halves(new)
            left = pltpu.roll(hz[0], turn(LANES - i), 1)
            right = pltpu.roll(hz[1], turn(LANES + last - i), 1)
            parts[0] = parts[0] + jnp.where(lane1 == 0, gain * left, 0.0)
            parts[-1] = parts[-1] + jnp.where(lane1 == last, gain * right, 0.0)
            new = jnp.concatenate(parts, 1) if len(parts) > 1 else parts[0]
            dst[i] = new
            return pack(l, i, new, acc) if onward is not None else acc

        acc = fix(0, zero_acc(l), hx[0])
        acc = fix(x - 1, acc, hx[1])
        started = onward[0]() if onward is not None else []
        acc = lax.fori_loop(1, x - 1, fix, acc)
        if onward is not None:
            store_acc(l, acc)
            started = started + onward[1]()
        return started

    def halves(v):
        return [v[:, k : k + LANES] for k in range(0, v.shape[1], LANES)]

    def restrict_y(ref, row_before):
        n = ref.shape[1] // 2
        parts = []
        first = lax.broadcasted_iota(jnp.int32, (n, LANES), 0) == 0
        for t, rim in enumerate(halves(row_before)):
            even = ref[t, pl.ds(0, n, stride=2), :]
            odd = ref[t, pl.ds(1, n, stride=2), :]
            below = jnp.where(first, rim, pltpu.roll(odd, 1, 0))
            parts.append(0.25 * below + 0.5 * even + 0.25 * odd)
        return jnp.concatenate(parts, 1) if len(parts) > 1 else parts[0]

    def restrict_down(l, d, mean):
        x, y, z = dims[l]
        zl = lane_pad(z)
        xc, yc, zc = dims[l + 1]
        zlc = lane_pad(zc)
        hx, hy, hz, hw = (b[f"r{a}{l}"] for a in "xyzw")
        s, t = b[f"S{l}"], b[f"T{l}"]
        m, n = b[f"M{l}"], b[f"N{l}"]
        lane = lax.broadcasted_iota(jnp.int32, (y + 8, LANES), 1)
        moved = pltpu.roll(hw[...], LANES - x, 1)
        rim = jnp.where(lane == LANES - 1, moved, hz[...])
        m[...] = dot_exact(rim, restrict_matrix(LANES, LANES, xc, LANES - 1))
        n[...] = m[pl.ds(0, y), :]
        even = n[pl.ds(0, yc, stride=2), :]
        odd = n[pl.ds(1, yc, stride=2), :]
        first = lax.broadcasted_iota(jnp.int32, (yc, LANES), 0) == 0
        below = jnp.where(first, m[pl.ds(y + 7, 1), :], pltpu.roll(odd, 1, 0))
        n[pl.ds(0, yc), :] = 0.25 * (0.25 * below + 0.5 * even + 0.25 * odd)

        def plane(i, before, before_row):
            dx = 0.25 * before + 0.5 * d[2 * i] + 0.25 * d[2 * i + 1]
            for k, part in enumerate(halves(dx)):
                s[k] = part
            rows = 0.25 * before_row + 0.5 * hy[pl.ds(2 * i, 1), :]
            rows = rows + 0.25 * hy[pl.ds(2 * i + 1, 1), :]
            t[i] = restrict_y(s, rows)

        def inner(i, _):
            plane(i, d[2 * i - 1], hy[pl.ds(2 * i - 1, 1), :])
            return 0

        plane(0, hx[...], hy[pl.ds(x + 7, 1), :])
        lax.fori_loop(1, xc, inner, 0)
        g, v = b[f"G{l + 1}"], b[f"A{l + 1}"]
        w = restrict_matrix(zl, zlc, zc)
        chunk = 8

        def multiply(k, _):
            rows = t[pl.ds(k * chunk, chunk)].reshape(chunk * yc, zl)
            g[pl.ds(k * chunk, chunk)] = dot_exact(rows, w).reshape(chunk, yc, zlc)
            return 0

        lax.fori_loop(0, xc // chunk, multiply, 0)
        lane_c = lax.broadcasted_iota(jnp.int32, (yc, zlc), 1)

        def finish(i):
            col = pltpu.roll(n[pl.ds(0, yc), :], turn(LANES - i), 1)
            new = g[i] + jnp.where(lane_c == 0, tile_up(col, zlc), 0.0)
            if mean is not None:
                new = new - mean
            g[i] = new
            new = (relax_weight / (6.0 * 0.25 ** (l + 1))) * new
            v[i] = new
            return new

        planes(l + 1, finish)

    def prolong_up(l, c, v, work, shift):
        x, y, z = dims[l]
        zl = lane_pad(z)
        xc, yc, zc = dims[l + 1]
        zlc = lane_pad(zc)
        hx, hy, hz, hw = (b[f"p{a}{l + 1}"] for a in "xyzw")
        s, t, th, ty = b[f"S{l}"], b[f"T{l}"], b[f"TH{l}"], b[f"TY{l}"]
        m = b[f"M{l + 1}"]
        lane = lax.broadcasted_iota(jnp.int32, (yc + 8, LANES), 1)
        m[...] = 0.5 * jnp.where(lane == xc, pltpu.roll(hw[...], xc, 1), hz[...])
        w = prolong_matrix(zlc, zl, zc)
        chunk = 8

        def multiply(k, _):
            rows = c[pl.ds(k * chunk, chunk)].reshape(chunk * yc, zlc)
            t[pl.ds(k * chunk, chunk)] = dot_exact(rows, w).reshape(chunk, yc, zl)
            return 0

        lax.fori_loop(0, xc // chunk, multiply, 0)
        th[...] = dot_exact(hx[...], w)
        ty[...] = dot_exact(hy[...], w)
        at_end = lane == LANES - 1
        final = lax.broadcasted_iota(jnp.int32, (yc, LANES), 0) == yc - 1

        def plane(i, values):
            add = pltpu.roll(m[...], turn(2 * LANES - 1 - i), 1)
            add = jnp.where(at_end, add, 0.0)
            rim = ty[pl.ds(i, 1), :]
            rims, parts = halves(rim), halves(values)
            parts[-1] = parts[-1] + add[:yc]
            rims[-1] = rims[-1] + add[yc : yc + 1]
            for k, (part, edge) in enumerate(zip(parts, rims)):
                above = jnp.where(final, edge, pltpu.roll(part, yc - 1, 0))
                s[k, pl.ds(0, yc, stride=2), :] = part
                s[k, pl.ds(1, yc, stride=2), :] = 0.5 * (part + above)
            full = [s[k] for k in range(len(parts))]
            work[i] = jnp.concatenate(full, 1) if len(full) > 1 else full[0]

        def spread(i, _):
            plane(i, t[i])
            return 0

        lax.fori_loop(0, xc, spread, 0)
        plane(xc, th[...])

        def add(i, acc):
            low, high = work[i], work[i + 1]
            if shift is not None:
                low, high = low - shift, high - shift
            even = v[2 * i] + low
            odd = v[2 * i + 1] + 0.5 * (low + high)
            v[2 * i] = even
            v[2 * i + 1] = odd
            return pack(l, 2 * i + 1, odd, pack(l, 2 * i, even, acc))

        store_acc(l, lax.fori_loop(0, xc, add, zero_acc(l)))

    st, sg = b["stats"], [b[f"sums{a}"] for a in range(3)]

    def spread_sums(a):
        return [
            copy(st.at[a], sg[a].at[j], tuple(j if i == a else 0 for i in range(3)))
            for j in range(1, counts[a])
        ]

    def gather_sums(a, copies):
        wait(copies)
        total = st[a]
        for j in range(1, counts[a]):
            total = total + sg[a][j]
        if a < 2:
            st[a + 1] = total
        return total

    x0, y0, z0 = dims[0]

    def folded(v):
        return jnp.sum(v.reshape(y0 // 8, 8, z0), 0)

    def first(i, carry):
        total, acc = carry
        v = u[i]
        return total + folded(v), pack(0, i, v, acc)

    none = jnp.zeros((8, z0), jnp.float32)
    total_u, acc = lax.fori_loop(0, x0, first, (none, zero_acc(0)))
    store_acc(0, acc)
    moving = both(exchange(0, 0, u))
    total_f = lax.fori_loop(0, x0, lambda i, t: t + folded(f[i]), none)
    st[0, 0] = total_u
    st[0, 1] = total_f
    sums = spread_sums(0)
    a0, b0, a1, b1 = b["A0"], b["B0"], b["A1"], b["B1"]
    a2, b2 = b["A2"], b["B2"]
    g1, g2 = b["G1"], b["G2"]
    moving = sweep(0, 0, moving, u, a0, f, exchange(0, 1, a0))
    gather_sums(0, sums)
    sums = spread_sums(1)
    moving = sweep(0, 1, moving, a0, b0, f, exchange(0, 2, b0))
    gather_sums(1, sums)
    sums = spread_sums(2)
    moving = sweep(0, 2, moving, b0, a0, f, corner_exchange("r", 0, a0), defect=True)
    total = gather_sums(2, sums)
    mean_u = jnp.sum(total[0]) * (1.0 / cells)
    mean_f = jnp.sum(total[1]) * (1.0 / cells)
    gain = relax_weight / 6.0
    wait(moving)
    restrict_down(0, a0, mean_f)

    moving = both(exchange(1, 0, a1))
    moving = sweep(1, 0, moving, a1, b1, g1, exchange(1, 1, b1))
    moving = sweep(1, 1, moving, b1, a1, g1, corner_exchange("r", 1, a1), defect=True)
    wait(moving)
    restrict_down(1, a1, None)

    v, w = a2, b2
    moving = both(exchange(2, 0, v))
    for k in range(COARSE_SWEEPS - 1):
        final = k == COARSE_SWEEPS - 2
        onward = corner_exchange("p", 2, w) if final else exchange(2, k + 1, w)
        moving = sweep(2, k, moving, v, w, g2, onward)
        v, w = w, v
    wait(moving)
    prolong_up(1, v, b1, a1, None)
    moving = both(exchange(1, 2, b1))
    moving = sweep(1, 2, moving, b1, a1, g1, exchange(1, 3, a1))
    moving = sweep(1, 3, moving, a1, b1, g1, corner_exchange("p", 1, b1))
    wait(moving)
    prolong_up(0, b1, b0, a0, mean_u + 2.0 * gain * mean_f)
    moving = both(exchange(0, 3, b0))
    moving = sweep(0, 3, moving, b0, a0, f, exchange(0, 4, a0), shift=gain * mean_f)
    sweep(0, 4, moving, a0, out, f, shift=gain * mean_f)


def solution(mesh):
    counts = tuple(mesh.shape[a] for a in AXES)

    def shards(right_side, initial_guess):
        shape = right_side.shape
        dims = tuple(tuple(n >> l for n in shape) for l in range(3))
        cells = float(right_side.size)
        for n in counts:
            cells *= n
        bufs = buffers(dims)
        bufs["stats"] = pltpu.VMEM((3, 2, 8, shape[2]), jnp.float32)
        for a in range(3):
            bufs[f"sums{a}"] = pltpu.VMEM((counts[a], 2, 8, shape[2]), jnp.float32)
        messages = 6 * (9 + COARSE_SWEEPS - 1) + 7 * 4 + sum(counts) - 3
        vmem = pl.BlockSpec(memory_space=pltpu.VMEM)
        return pl.pallas_call(
            functools.partial(kernel, dims, counts, tuple(bufs), cells),
            out_shape=jax.ShapeDtypeStruct(shape, jnp.float32),
            in_specs=[vmem, vmem],
            out_specs=vmem,
            scratch_shapes=list(bufs.values())
            + [pltpu.SemaphoreType.DMA((messages,)), pltpu.SemaphoreType.DMA((messages,))],
            compiler_params=pltpu.CompilerParams(
                collective_id=0, has_side_effects=True, vmem_limit_bytes=48 * 1024 * 1024
            ),
        )(initial_guess, right_side)

    placed = (P(*AXES), P(*AXES))
    return jax.shard_map(
        shards, mesh=mesh, in_specs=placed, out_specs=P(*AXES), check_vma=False
    )
```

```python
import functools
import itertools

import jax
import jax.numpy as jnp
from jax import lax
from jax.experimental import pallas as pl
from jax.experimental.pallas import tpu as pltpu
from jax.sharding import PartitionSpec as P

COARSE_SWEEPS = 6
LANES = 128
AXES = ("gx", "gy", "gz")
relax_weight = 0.8


def dot_exact(a, w):
    hi = a.astype(jnp.bfloat16)
    rest = a - hi.astype(jnp.float32)
    mid = rest.astype(jnp.bfloat16)
    low = (rest - mid.astype(jnp.float32)).astype(jnp.bfloat16)
    dot = functools.partial(jnp.dot, preferred_element_type=jnp.float32)
    return dot(hi, w) + (dot(mid, w) + dot(low, w))


def iotas(shape):
    return (
        lax.broadcasted_iota(jnp.int32, shape, 0),
        lax.broadcasted_iota(jnp.int32, shape, 1),
    )


def restrict_matrix(rows, cols, count, wrap=None):
    r, c = iotas((rows, cols))
    w = jnp.where(r == 2 * c, 0.5, 0.0) + jnp.where(jnp.abs(r - 2 * c) == 1, 0.25, 0.0)
    w = jnp.where((c < count) & (r < 2 * count), w, 0.0)
    if wrap is not None:
        w = w + jnp.where((r == wrap) & (c == 0), 0.25, 0.0)
    return w.astype(jnp.bfloat16)


def prolong_matrix(rows, cols, count):
    r, c = iotas((rows, cols))
    w = jnp.where(c == 2 * r, 1.0, 0.0)
    w = w + jnp.where((c == 2 * r + 1) | (c == 2 * r - 1), 0.5, 0.0)
    return jnp.where(r < count, w, 0.0).astype(jnp.bfloat16)


def lane_pad(z):
    return max(z, LANES)


def turn(by):
    return by % LANES if isinstance(by, int) else lax.rem(by, LANES)


def tile_up(h, width):
    return jnp.concatenate([h] * (width // LANES), 1) if width > LANES else h


def buffers(dims):
    f32 = jnp.float32
    out = {}
    rounds = (5, 4, COARSE_SWEEPS - 1)
    for l, (x, y, z) in enumerate(dims):
        zl = lane_pad(z)
        for name in "AB":
            out[f"{name}{l}"] = (x, y, zl)
        if l:
            out[f"G{l}"] = (x, y, zl)
        out[f"yp{l}"] = (2, x, zl)
        out[f"zp{l}"] = (2, y, LANES)
        out[f"hx{l}"] = (rounds[l], 2, y, zl)
        out[f"hy{l}"] = (rounds[l], 2, x, zl)
        out[f"hz{l}"] = (rounds[l], 2, y, LANES)
        for kind in (["r"] if l < 2 else []) + (["p"] if l else []):
            out[f"{kind}x{l}"] = (y, zl)
            out[f"{kind}y{l}"] = (x + 8, zl)
            out[f"{kind}z{l}"] = (y + 8, LANES)
            out[f"{kind}w{l}"] = (y + 8, LANES)
        if l < 2:
            out[f"T{l}"] = (x // 2, y // 2, zl)
            out[f"S{l}"] = (zl // LANES, y, LANES)
            out[f"TH{l}"] = (y // 2, zl)
            out[f"TY{l}"] = (x // 2 + 8, zl)
        out[f"M{l}"] = (y + 8, LANES)
        out[f"N{l}"] = (y, LANES)
    return {k: pltpu.VMEM(v, f32) for k, v in out.items()}


def kernel(dims, counts, names, cells, u_far, f_far, out, *scratch):
    b = dict(zip(names, scratch[:-3]))
    send_sem, recv_sem, load_sem = scratch[-3:]
    u, f = b["u"], b["f"]
    load_u = pltpu.make_async_copy(u_far, u, load_sem.at[0])
    load_f = pltpu.make_async_copy(f_far, f, load_sem.at[1])
    load_u.start()
    load_f.start()
    here = {a: lax.axis_index(a) for a in AXES}
    serial = itertools.count()

    def device(offset):
        return tuple(lax.rem(here[a] + (o % n), n) for a, o, n in zip(AXES, offset, counts))

    def copy(src, dst, offset):
        k = next(serial)
        c = pltpu.make_async_remote_copy(
            src_ref=src,
            dst_ref=dst,
            send_sem=send_sem.at[k],
            recv_sem=recv_sem.at[k],
            device_id=device(offset),
            device_id_type=pl.DeviceIdType.MESH,
        )
        c.start()
        return c

    def wait(copies):
        for c in copies:
            c.wait()

    offsets = []
    for sign in (1, -1):
        for o in itertools.product((0, 1), repeat=3):
            if any(o):
                offsets.append(tuple(sign * v for v in o))
    for a in range(3):
        for j in range(2, counts[a] - 1):
            offsets.append(tuple(j if i == a else 0 for i in range(3)))
    barrier = pltpu.get_barrier_semaphore()
    for o in offsets:
        pl.semaphore_signal(
            barrier, inc=1, device_id=device(o), device_id_type=pl.DeviceIdType.MESH
        )
    pl.semaphore_wait(barrier, len(offsets))

    def exchange(l, r, v):
        x = dims[l][0]
        hx, hy, hz = (b[f"h{a}{l}"] for a in "xyz")
        yp, zp = b[f"yp{l}"], b[f"zp{l}"]

        def early():
            return [
                copy(v.at[x - 1], hx.at[r, 0], (1, 0, 0)),
                copy(v.at[0], hx.at[r, 1], (-1, 0, 0)),
            ]

        def late():
            return [
                copy(yp.at[1], hy.at[r, 0], (0, 1, 0)),
                copy(yp.at[0], hy.at[r, 1], (0, -1, 0)),
                copy(zp.at[1], hz.at[r, 0], (0, 0, 1)),
                copy(zp.at[0], hz.at[r, 1], (0, 0, -1)),
            ]

        return early, late

    def corner_exchange(kind, l, v):
        x, y, _ = dims[l]
        hi = kind == "r"
        s = 1 if hi else -1
        side = 1 if hi else 0
        yp, zp = b[f"yp{l}"].at[side], b[f"zp{l}"].at[side]
        hx, hy, hz, hw = (b[f"{kind}{a}{l}"] for a in "xyzw")
        ye = yp.at[pl.ds(x - 8 if hi else 0, 8)]
        ze = zp.at[pl.ds(y - 8 if hi else 0, 8)]

        def early():
            return [copy(v.at[x - 1 if hi else 0], hx, (s, 0, 0))]

        def late():
            return [
                copy(ze, hw.at[pl.ds(y, 8)], (s, s, s)),
                copy(zp, hw.at[pl.ds(0, y)], (s, 0, s)),
                copy(ze, hz.at[pl.ds(y, 8)], (0, s, s)),
                copy(ye, hy.at[pl.ds(x, 8)], (s, s, 0)),
                copy(yp, hy.at[pl.ds(0, x)], (0, s, 0)),
                copy(zp, hz.at[pl.ds(0, y)], (0, 0, s)),
            ]

        return early, late

    def both(parts):
        return parts[0]() + parts[1]()

    def zero_acc(l):
        z = jnp.zeros((dims[l][1], LANES), jnp.float32)
        return (z, z)

    def pack(l, x, new, acc):
        _, y, z = dims[l]
        yp = b[f"yp{l}"]
        yp[0, pl.ds(x, 1), :] = new[:1]
        yp[1, pl.ds(x, 1), :] = new[y - 1 :]
        lane = lax.broadcasted_iota(jnp.int32, (y, LANES), 1)
        last = (z - 1) % LANES
        low = pltpu.roll(new[:, :LANES], x, 1)
        high = pltpu.roll(new[:, -LANES:], turn(x + (LANES - last)), 1)
        return (jnp.where(lane == x, low, acc[0]), jnp.where(lane == x, high, acc[1]))

    def store_acc(l, acc):
        b[f"zp{l}"][0] = acc[0]
        b[f"zp{l}"][1] = acc[1]

    def planes(l, body, packed=True):
        def step(i, acc):
            new = body(i)
            return pack(l, i, new, acc) if packed else acc

        acc = lax.fori_loop(0, dims[l][0], step, zero_acc(l))
        if packed:
            store_acc(l, acc)

    def sweep(l, r, moving, src, dst, g, onward=None, defect=False, shift=None):
        x, y, z = dims[l]
        zl = lane_pad(z)
        scale = 0.25**l
        hx, hy, hz = (b[f"h{a}{l}"].at[r] for a in "xyz")
        row, lane = iotas((y, zl))
        last = (z - 1) % LANES
        gain = scale if defect else relax_weight / 6.0

        def plane(i, around):
            c = src[i]
            up = jnp.where(row == 0, 0.0, pltpu.roll(c, 1, 0))
            down = jnp.where(row == y - 1, 0.0, pltpu.roll(c, y - 1, 0))
            left = jnp.where(lane == 0, 0.0, pltpu.roll(c, 1, 1))
            right = jnp.where(lane == z - 1, 0.0, pltpu.roll(c, zl - 1, 1))
            beside = around + (up + down) + (left + right)
            if defect:
                new = g[i] - scale * (6.0 * c - beside)
            else:
                new = (1.0 - relax_weight) * c + (relax_weight / 6.0) * beside
                new = new + (relax_weight / (6.0 * scale)) * g[i]
                if shift is not None:
                    new = new - shift
            dst[i] = new

        def inner(i, _):
            plane(i, src[i - 1] + src[i + 1])
            return 0

        plane(0, src[1])
        lax.fori_loop(1, x - 1, inner, 0)
        plane(x - 1, src[x - 2])
        wait(moving)
        row8 = lax.broadcasted_iota(jnp.int32, (8, zl), 0)
        lane1 = lax.broadcasted_iota(jnp.int32, (y, LANES), 1)

        def fix(i, acc, beyond=None):
            new = dst[i]
            if beyond is not None:
                new = new + gain * beyond
            top = new[:8] + jnp.where(row8 == 0, gain * hy[0, pl.ds(i, 1), :], 0.0)
            new = jnp.concatenate([top, new[8:]], 0) if y > 8 else top
            end = new[y - 8 :] + jnp.where(row8 == 7, gain * hy[1, pl.ds(i, 1), :], 0.0)
            new = jnp.concatenate([new[: y - 8], end], 0) if y > 8 else end
            parts = halves(new)
            left = pltpu.roll(hz[0], turn(LANES - i), 1)
            right = pltpu.roll(hz[1], turn(LANES + last - i), 1)
            parts[0] = parts[0] + jnp.where(lane1 == 0, gain * left, 0.0)
            parts[-1] = parts[-1] + jnp.where(lane1 == last, gain * right, 0.0)
            new = jnp.concatenate(parts, 1) if len(parts) > 1 else parts[0]
            dst[i] = new
            return pack(l, i, new, acc) if onward is not None else acc

        acc = fix(0, zero_acc(l), hx[0])
        acc = fix(x - 1, acc, hx[1])
        started = onward[0]() if onward is not None else []
        acc = lax.fori_loop(1, x - 1, fix, acc)
        if onward is not None:
            store_acc(l, acc)
            started = started + onward[1]()
        return started

    def halves(v):
        return [v[:, k : k + LANES] for k in range(0, v.shape[1], LANES)]

    def restrict_y(ref, row_before):
        n = ref.shape[1] // 2
        parts = []
        first = lax.broadcasted_iota(jnp.int32, (n, LANES), 0) == 0
        for t, rim in enumerate(halves(row_before)):
            even = ref[t, pl.ds(0, n, stride=2), :]
            odd = ref[t, pl.ds(1, n, stride=2), :]
            below = jnp.where(first, rim, pltpu.roll(odd, 1, 0))
            parts.append(0.25 * below + 0.5 * even + 0.25 * odd)
        return jnp.concatenate(parts, 1) if len(parts) > 1 else parts[0]

    def restrict_down(l, d, mean):
        x, y, z = dims[l]
        zl = lane_pad(z)
        xc, yc, zc = dims[l + 1]
        zlc = lane_pad(zc)
        hx, hy, hz, hw = (b[f"r{a}{l}"] for a in "xyzw")
        s, t = b[f"S{l}"], b[f"T{l}"]
        m, n = b[f"M{l}"], b[f"N{l}"]
        lane = lax.broadcasted_iota(jnp.int32, (y + 8, LANES), 1)
        moved = pltpu.roll(hw[...], LANES - x, 1)
        rim = jnp.where(lane == LANES - 1, moved, hz[...])
        m[...] = dot_exact(rim, restrict_matrix(LANES, LANES, xc, LANES - 1))
        n[...] = m[pl.ds(0, y), :]
        even = n[pl.ds(0, yc, stride=2), :]
        odd = n[pl.ds(1, yc, stride=2), :]
        first = lax.broadcasted_iota(jnp.int32, (yc, LANES), 0) == 0
        below = jnp.where(first, m[pl.ds(y + 7, 1), :], pltpu.roll(odd, 1, 0))
        n[pl.ds(0, yc), :] = 0.25 * (0.25 * below + 0.5 * even + 0.25 * odd)

        def plane(i, before, before_row):
            dx = 0.25 * before + 0.5 * d[2 * i] + 0.25 * d[2 * i + 1]
            for k, part in enumerate(halves(dx)):
                s[k] = part
            rows = 0.25 * before_row + 0.5 * hy[pl.ds(2 * i, 1), :]
            rows = rows + 0.25 * hy[pl.ds(2 * i + 1, 1), :]
            t[i] = restrict_y(s, rows)

        def inner(i, _):
            plane(i, d[2 * i - 1], hy[pl.ds(2 * i - 1, 1), :])
            return 0

        plane(0, hx[...], hy[pl.ds(x + 7, 1), :])
        lax.fori_loop(1, xc, inner, 0)
        g, v = b[f"G{l + 1}"], b[f"A{l + 1}"]
        w = restrict_matrix(zl, zlc, zc)
        chunk = 8

        def multiply(k, _):
            rows = t[pl.ds(k * chunk, chunk)].reshape(chunk * yc, zl)
            g[pl.ds(k * chunk, chunk)] = dot_exact(rows, w).reshape(chunk, yc, zlc)
            return 0

        lax.fori_loop(0, xc // chunk, multiply, 0)
        lane_c = lax.broadcasted_iota(jnp.int32, (yc, zlc), 1)

        def finish(i):
            col = pltpu.roll(n[pl.ds(0, yc), :], turn(LANES - i), 1)
            new = g[i] + jnp.where(lane_c == 0, tile_up(col, zlc), 0.0)
            if mean is not None:
                new = new - mean
            g[i] = new
            new = (relax_weight / (6.0 * 0.25 ** (l + 1))) * new
            v[i] = new
            return new

        planes(l + 1, finish)

    def prolong_up(l, c, v, work, shift):
        x, y, z = dims[l]
        zl = lane_pad(z)
        xc, yc, zc = dims[l + 1]
        zlc = lane_pad(zc)
        hx, hy, hz, hw = (b[f"p{a}{l + 1}"] for a in "xyzw")
        s, t, th, ty = b[f"S{l}"], b[f"T{l}"], b[f"TH{l}"], b[f"TY{l}"]
        m = b[f"M{l + 1}"]
        lane = lax.broadcasted_iota(jnp.int32, (yc + 8, LANES), 1)
        m[...] = 0.5 * jnp.where(lane == xc, pltpu.roll(hw[...], xc, 1), hz[...])
        w = prolong_matrix(zlc, zl, zc)
        chunk = 8

        def multiply(k, _):
            rows = c[pl.ds(k * chunk, chunk)].reshape(chunk * yc, zlc)
            t[pl.ds(k * chunk, chunk)] = dot_exact(rows, w).reshape(chunk, yc, zl)
            return 0

        lax.fori_loop(0, xc // chunk, multiply, 0)
        th[...] = dot_exact(hx[...], w)
        ty[...] = dot_exact(hy[...], w)
        at_end = lane == LANES - 1
        final = lax.broadcasted_iota(jnp.int32, (yc, LANES), 0) == yc - 1

        def plane(i, values):
            add = pltpu.roll(m[...], turn(2 * LANES - 1 - i), 1)
            add = jnp.where(at_end, add, 0.0)
            rim = ty[pl.ds(i, 1), :]
            rims, parts = halves(rim), halves(values)
            parts[-1] = parts[-1] + add[:yc]
            rims[-1] = rims[-1] + add[yc : yc + 1]
            for k, (part, edge) in enumerate(zip(parts, rims)):
                above = jnp.where(final, edge, pltpu.roll(part, yc - 1, 0))
                s[k, pl.ds(0, yc, stride=2), :] = part
                s[k, pl.ds(1, yc, stride=2), :] = 0.5 * (part + above)
            full = [s[k] for k in range(len(parts))]
            work[i] = jnp.concatenate(full, 1) if len(full) > 1 else full[0]

        def spread(i, _):
            plane(i, t[i])
            return 0

        lax.fori_loop(0, xc, spread, 0)
        plane(xc, th[...])

        def add(i, acc):
            low, high = work[i], work[i + 1]
            if shift is not None:
                low, high = low - shift, high - shift
            even = v[2 * i] + low
            odd = v[2 * i + 1] + 0.5 * (low + high)
            v[2 * i] = even
            v[2 * i + 1] = odd
            return pack(l, 2 * i + 1, odd, pack(l, 2 * i, even, acc))

        store_acc(l, lax.fori_loop(0, xc, add, zero_acc(l)))

    st, sg = b["stats"], [b[f"sums{a}"] for a in range(3)]

    def spread_sums(a):
        return [
            copy(st.at[a], sg[a].at[j], tuple(j if i == a else 0 for i in range(3)))
            for j in range(1, counts[a])
        ]

    def gather_sums(a, copies):
        wait(copies)
        total = st[a]
        for j in range(1, counts[a]):
            total = total + sg[a][j]
        if a < 2:
            st[a + 1] = total
        return total

    x0, y0, z0 = dims[0]

    def folded(v):
        return jnp.sum(v.reshape(y0 // 8, 8, z0), 0)

    def first(i, carry):
        total, acc = carry
        v = u[i]
        return total + folded(v), pack(0, i, v, acc)

    none = jnp.zeros((8, z0), jnp.float32)
    load_u.wait()
    total_u, acc = lax.fori_loop(0, x0, first, (none, zero_acc(0)))
    store_acc(0, acc)
    moving = both(exchange(0, 0, u))
    load_f.wait()
    total_f = lax.fori_loop(0, x0, lambda i, t: t + folded(f[i]), none)
    st[0, 0] = total_u
    st[0, 1] = total_f
    sums = spread_sums(0)
    a0, b0, a1, b1 = b["A0"], b["B0"], b["A1"], b["B1"]
    a2, b2 = b["A2"], b["B2"]
    g1, g2 = b["G1"], b["G2"]
    moving = sweep(0, 0, moving, u, a0, f, exchange(0, 1, a0))
    gather_sums(0, sums)
    sums = spread_sums(1)
    moving = sweep(0, 1, moving, a0, b0, f, exchange(0, 2, b0))
    gather_sums(1, sums)
    sums = spread_sums(2)
    moving = sweep(0, 2, moving, b0, a0, f, corner_exchange("r", 0, a0), defect=True)
    total = gather_sums(2, sums)
    mean_u = jnp.sum(total[0]) * (1.0 / cells)
    mean_f = jnp.sum(total[1]) * (1.0 / cells)
    gain = relax_weight / 6.0
    wait(moving)
    restrict_down(0, a0, mean_f)

    moving = both(exchange(1, 0, a1))
    moving = sweep(1, 0, moving, a1, b1, g1, exchange(1, 1, b1))
    moving = sweep(1, 1, moving, b1, a1, g1, corner_exchange("r", 1, a1), defect=True)
    wait(moving)
    restrict_down(1, a1, None)

    v, w = a2, b2
    moving = both(exchange(2, 0, v))
    for k in range(COARSE_SWEEPS - 1):
        final = k == COARSE_SWEEPS - 2
        onward = corner_exchange("p", 2, w) if final else exchange(2, k + 1, w)
        moving = sweep(2, k, moving, v, w, g2, onward)
        v, w = w, v
    wait(moving)
    prolong_up(1, v, b1, a1, None)
    moving = both(exchange(1, 2, b1))
    moving = sweep(1, 2, moving, b1, a1, g1, exchange(1, 3, a1))
    moving = sweep(1, 3, moving, a1, b1, g1, corner_exchange("p", 1, b1))
    wait(moving)
    prolong_up(0, b1, b0, a0, mean_u + 2.0 * gain * mean_f)
    moving = both(exchange(0, 3, b0))
    moving = sweep(0, 3, moving, b0, a0, f, exchange(0, 4, a0), shift=gain * mean_f)
    sweep(0, 4, moving, a0, out, f, shift=gain * mean_f)


def solution(mesh):
    counts = tuple(mesh.shape[a] for a in AXES)

    def shards(right_side, initial_guess):
        shape = right_side.shape
        dims = tuple(tuple(n >> l for n in shape) for l in range(3))
        cells = float(right_side.size)
        for n in counts:
            cells *= n
        bufs = buffers(dims)
        bufs["u"] = pltpu.VMEM(shape, jnp.float32)
        bufs["f"] = pltpu.VMEM(shape, jnp.float32)
        bufs["stats"] = pltpu.VMEM((3, 2, 8, shape[2]), jnp.float32)
        for a in range(3):
            bufs[f"sums{a}"] = pltpu.VMEM((counts[a], 2, 8, shape[2]), jnp.float32)
        messages = 6 * (9 + COARSE_SWEEPS - 1) + 7 * 4 + sum(counts) - 3
        vmem = pl.BlockSpec(memory_space=pltpu.VMEM)
        return pl.pallas_call(
            functools.partial(kernel, dims, counts, tuple(bufs), cells),
            out_shape=jax.ShapeDtypeStruct(shape, jnp.float32),
            in_specs=[pl.BlockSpec(memory_space=pl.ANY)] * 2,
            out_specs=vmem,
            scratch_shapes=list(bufs.values())
            + [pltpu.SemaphoreType.DMA((n,)) for n in (messages, messages, 2)],
            compiler_params=pltpu.CompilerParams(
                collective_id=0, has_side_effects=True, vmem_limit_bytes=48 * 1024 * 1024
            ),
        )(initial_guess, right_side)

    placed = (P(*AXES), P(*AXES))
    return jax.shard_map(
        shards, mesh=mesh, in_specs=placed, out_specs=P(*AXES), check_vma=False
    )
```
